8 devices in a mesh: dp: 1 (over z), ep: 8 (over y, x, core).
Axes of the slice: x: 2, y: 2, z: 1, core: 2. Of those that a mesh axis runs over, the one named last changes fastest.
Arguments:
- resid_in: bfloat16 [4096, 2560], P(('dp', 'ep'))
- expert_ids: int32 [4096, 6], P(('dp', 'ep'))
- priority: int32 [4096, 6], P(('dp', 'ep'))
- norm_gain: float32 [2560], replicated
- router_w: bfloat16 [2560, 64], replicated
- shared_w1: bfloat16 [2560, 3072], replicated
- shared_w3: bfloat16 [2560, 3072], replicated
- shared_w2: bfloat16 [3072, 2560], replicated
- expert_w1: bfloat16 [64, 2560, 1536], P('ep')
- expert_w3: bfloat16 [64, 2560, 1536], P('ep')
- expert_w2: bfloat16 [64, 1536, 2560], P('ep')
Outputs:
- output: bfloat16 [4096, 2560], P(('dp', 'ep'))
All inputs are finite; a program needn't handle non-finite values.
Results may differ from the reference program's by a relative error of at most 0.00677964.
Values are sent between devices in bfloat16 or wider.
A program may use at most 1 GiB of HBM per device.

```python
import math
import jax
import jax.numpy as jnp
from jax import lax

HIDDEN = 2560
EXPERTS = 64
TOP_K = 6
EXPERT_FF = 1536
SHARED_FF = 3072
GROUPS = 1
TOP_GROUPS = 1
EP_SIZE = 8
TOKENS = 4096
CAPACITY = 3072

NORM_EPS = 1e-6
ROUTE_SCALE = 16.0


def draw_routing(route_key):
    key_group, key_score, key_hot, key_prio = jax.random.split(route_key, 4)
    group_width = EXPERTS // GROUPS
    n_cand = TOP_GROUPS * group_width
    local_experts = EXPERTS // EP_SIZE
    hot_range = 1280 * TOP_K // n_cand
    hot_dev = jax.random.permutation(key_hot, EP_SIZE) * hot_range // EP_SIZE
    group_score = jax.random.randint(key_group, (TOKENS, GROUPS), 0, 1 << 20) * GROUPS + jnp.arange(GROUPS)
    group_pick = lax.top_k(group_score, TOP_GROUPS)[1]
    cand_ids = (group_pick[:, :, None] * group_width + jnp.arange(group_width)).reshape(TOKENS, n_cand)
    score_noise = jax.random.randint(key_score, (TOKENS, n_cand), 0, 1024)
    cand_score = (score_noise + hot_dev[cand_ids // local_experts]) * n_cand + jnp.arange(n_cand)
    pick_idx = lax.top_k(cand_score, TOP_K)[1]
    expert_ids = jnp.take_along_axis(cand_ids, pick_idx, axis=1).astype(jnp.int32)
    priority = jax.random.permutation(key_prio, TOKENS * TOP_K).reshape(TOKENS, TOP_K).astype(jnp.int32)
    return expert_ids, priority


def setup_inputs(seed: int = 0, part: int = 0) -> dict:
    root_key = jax.random.key(seed)
    resid_key, route_key = jax.random.split(jax.random.fold_in(root_key, part))
    weight_keys = jax.random.split(jax.random.fold_in(root_key, 1 << 30), 8)
    expert_ids, priority = draw_routing(route_key)
    down_gain = EXPERTS / (10.0 * math.sqrt(TOP_K))
    return dict(
        resid_in=jax.random.normal(resid_key, (TOKENS, HIDDEN), jnp.float32).astype(jnp.bfloat16),
        expert_ids=expert_ids,
        priority=priority,
        norm_gain=1.0 + 0.3 * jax.random.normal(weight_keys[0], (HIDDEN,), jnp.float32),
        router_w=(0.5 * HIDDEN ** -0.5 * jax.random.normal(weight_keys[1], (HIDDEN, EXPERTS), jnp.float32)).astype(jnp.bfloat16),
        shared_w1=(HIDDEN ** -0.5 * jax.random.normal(weight_keys[2], (HIDDEN, SHARED_FF), jnp.float32)).astype(jnp.bfloat16),
        shared_w3=(HIDDEN ** -0.5 * jax.random.normal(weight_keys[3], (HIDDEN, SHARED_FF), jnp.float32)).astype(jnp.bfloat16),
        shared_w2=(SHARED_FF ** -0.5 * jax.random.normal(weight_keys[4], (SHARED_FF, HIDDEN), jnp.float32)).astype(jnp.bfloat16),
        expert_w1=(HIDDEN ** -0.5 * jax.random.normal(weight_keys[5], (EXPERTS, HIDDEN, EXPERT_FF), jnp.float32)).astype(jnp.bfloat16),
        expert_w3=(HIDDEN ** -0.5 * jax.random.normal(weight_keys[6], (EXPERTS, HIDDEN, EXPERT_FF), jnp.float32)).astype(jnp.bfloat16),
        expert_w2=(down_gain * EXPERT_FF ** -0.5 * jax.random.normal(weight_keys[7], (EXPERTS, EXPERT_FF, HIDDEN), jnp.float32)).astype(jnp.bfloat16),
    )


def swiglu_ffn(normed, w_gate, w_up, w_down):
    up_a = jnp.dot(normed, w_gate, preferred_element_type=jnp.float32)
    up_b = jnp.dot(normed, w_up, preferred_element_type=jnp.float32)
    hidden_act = (jax.nn.silu(up_a) * up_b).astype(jnp.bfloat16)
    return jnp.dot(hidden_act, w_down, preferred_element_type=jnp.float32).astype(jnp.bfloat16)


def keep_mask(expert_ids, priority):
    n_assign = TOKENS * TOP_K
    owners = (expert_ids // (EXPERTS // EP_SIZE)).reshape(n_assign)
    prio_flat = priority.reshape(n_assign)
    owner_by_rank = jnp.zeros((n_assign,), jnp.int32).at[prio_flat].set(owners)
    dest_hits = (owner_by_rank[:, None] == jnp.arange(EP_SIZE, dtype=jnp.int32)).astype(jnp.int32)
    before = jnp.cumsum(dest_hits, axis=0) - dest_hits
    rank_by_prio = jnp.sum(before * dest_hits, axis=1)
    return (rank_by_prio[prio_flat] < CAPACITY).reshape(TOKENS, TOP_K)


def routed_sum(normed, expert_ids, flat_gates, expert_w1, expert_w3, expert_w2):
    n_assign = TOKENS * TOP_K
    row_block = max(8, n_assign // (32 * EXPERTS) * 8)
    n_blocks = n_assign // row_block + EXPERTS + 1
    flat_ids = expert_ids.reshape(n_assign)
    sort_order = jnp.argsort(flat_ids * n_assign + jnp.arange(n_assign, dtype=jnp.int32)).astype(jnp.int32)
    counts = jax.ops.segment_sum(jnp.ones((n_assign,), jnp.int32), flat_ids, num_segments=EXPERTS)
    padded = (counts + row_block - 1) // row_block * row_block
    pad_start = jnp.cumsum(padded) - padded
    sort_start = jnp.cumsum(counts) - counts
    sorted_ids = flat_ids[sort_order]
    dest_row = pad_start[sorted_ids] + jnp.arange(n_assign, dtype=jnp.int32) - sort_start[sorted_ids]
    row_src = jnp.full((n_blocks * row_block,), n_assign, jnp.int32).at[dest_row].set(sort_order)
    block_first = jnp.arange(n_blocks, dtype=jnp.int32) * row_block
    block_expert = jnp.sum((pad_start[None, :] <= block_first[:, None]).astype(jnp.int32), axis=1) - 1
    normed_pad = jnp.concatenate([normed, jnp.zeros((1, HIDDEN), normed.dtype)], axis=0)
    gates_pad = jnp.concatenate([flat_gates, jnp.zeros((1,), flat_gates.dtype)])

    def one_block(routed_acc, block_args):
        src_rows, expert = block_args
        tok_rows = src_rows // TOP_K
        expert_out = swiglu_ffn(normed_pad[tok_rows], expert_w1[expert], expert_w3[expert], expert_w2[expert])
        weighted = expert_out.astype(jnp.float32) * gates_pad[src_rows][:, None]
        return routed_acc.at[tok_rows].add(weighted), None

    routed_acc = lax.scan(one_block, jnp.zeros((TOKENS + 1, HIDDEN), jnp.float32), (row_src.reshape(n_blocks, row_block), block_expert))[0]
    return routed_acc[:TOKENS]


def reference(resid_in, expert_ids, priority, norm_gain, router_w, shared_w1, shared_w3, shared_w2, expert_w1, expert_w3, expert_w2):
    resid32 = resid_in.astype(jnp.float32)
    inv_rms = lax.rsqrt(jnp.mean(resid32 * resid32, axis=1, keepdims=True) + NORM_EPS)
    normed = (resid32 * inv_rms * norm_gain).astype(jnp.bfloat16)
    gate_probs = jax.nn.softmax(jnp.dot(normed, router_w, preferred_element_type=jnp.float32), axis=1)
    gate_vals = ROUTE_SCALE * jnp.take_along_axis(gate_probs, expert_ids, axis=1)
    kept_mask = keep_mask(expert_ids, priority)
    flat_gates = jnp.where(kept_mask, gate_vals, 0.0).reshape(TOKENS * TOP_K)
    shared_out = swiglu_ffn(normed, shared_w1, shared_w3, shared_w2)
    routed = routed_sum(normed, expert_ids, flat_gates, expert_w1, expert_w3, expert_w2)
    return (resid32 + shared_out.astype(jnp.float32) + routed).astype(jnp.bfloat16)
```

```python
import functools
import jax
import jax.numpy as jnp
from jax import lax
from jax.experimental import pallas as pl
from jax.experimental.pallas import tpu as pltpu
from jax.sharding import PartitionSpec as P

NORM_EPS = 1e-6
ROUTE_SCALE = 16.0
PRIO_BITS = 15
PRIO_MASK = (1 << PRIO_BITS) - 1

GROUPS = ((0, 1), (2, 3, 4), (5, 6, 7))
STARTS = (0, 96, 240)
BUCKET = 448
SPILL = 64
ROWS_MAX = 480
SEG_MAX = 80
SEG_WIN = 96
F_TILE = 512


def window(c):
    end = STARTS[c + 1] if c + 1 < len(STARTS) else BUCKET
    return STARTS[c], end - STARTS[c]


def grouped_ffn(row_inputs, group_sizes, slot_valid, expert_w1, expert_w3, expert_w2):
    up_a = lax.ragged_dot(row_inputs, expert_w1, group_sizes, preferred_element_type=jnp.float32)
    up_b = lax.ragged_dot(row_inputs, expert_w3, group_sizes, preferred_element_type=jnp.float32)
    hidden_act = (jax.nn.silu(up_a) * up_b).astype(jnp.bfloat16)
    expert_out = lax.ragged_dot(hidden_act, expert_w2, group_sizes, preferred_element_type=jnp.float32).astype(jnp.bfloat16)
    return jnp.where(slot_valid[:, None], expert_out.astype(jnp.float32), 0.0)


def local_keep(flat_ids, prio_flat, local_experts, capacity, my_index):
    n_assign = flat_ids.shape[0]
    mine_int = (flat_ids // local_experts == my_index).astype(jnp.int32)
    by_rank = jnp.zeros((n_assign,), jnp.int32).at[prio_flat].set(mine_int)
    before = jnp.cumsum(by_rank) - by_rank
    return (mine_int > 0) & (before[prio_flat] < capacity)


def slot_layout(flat_ids, mine_kept, local_experts, capacity, my_index):
    n_assign = flat_ids.shape[0]
    local_e = flat_ids - my_index * local_experts
    sort_key = jnp.where(mine_kept, local_e, local_experts) * n_assign + jnp.arange(n_assign, dtype=jnp.int32)
    slot_order = jnp.argsort(sort_key)[:capacity]
    group_sizes = jax.ops.segment_sum(mine_kept.astype(jnp.int32), jnp.where(mine_kept, local_e, 0), num_segments=local_experts)
    return slot_order, group_sizes, mine_kept[slot_order]


def general_path(acc0, all_normed, expert_ids, priority, gates_by_expert, my_index, expert_w1, expert_w3, expert_w2, ep_size):
    tok_local, top_k = expert_ids.shape
    local_experts = expert_w1.shape[0]
    capacity = tok_local * top_k
    gate_vals = jnp.take_along_axis(gates_by_expert, expert_ids, axis=1)
    all_ids = lax.all_gather(expert_ids, 'ep', tiled=True).reshape(-1)
    all_prio = lax.all_gather(priority, 'ep', tiled=True).reshape(-1)
    all_gates = lax.all_gather(gate_vals, 'ep', tiled=True).reshape(-1)
    mine_kept = local_keep(all_ids, all_prio, local_experts, capacity, my_index)
    slot_order, group_sizes, slot_valid = slot_layout(all_ids, mine_kept, local_experts, capacity, my_index)
    tok_of = slot_order // top_k
    expert_out = grouped_ffn(all_normed[tok_of], group_sizes, slot_valid, expert_w1, expert_w3, expert_w2)
    weighted = expert_out * all_gates[slot_order][:, None]
    token_sums = jax.ops.segment_sum(weighted, tok_of, num_segments=tok_local * ep_size)
    routed = lax.psum_scatter(token_sums, 'ep', scatter_dimension=0, tiled=True)
    return (acc0 + routed).astype(jnp.bfloat16)


def route_kernel(ep, n_loc, capacity, me_ref, keys_ref, own_ref, qx_ref, qt_ref, tab_ref):
    me = me_ref[0]
    tok = own_ref.shape[1]
    kpad = own_ref.shape[0]
    n_all = ep * n_loc
    log_loc = n_loc.bit_length() - 1
    keys = keys_ref[...]
    ids = (keys >> PRIO_BITS) ^ (me * n_loc)
    prio = keys & PRIO_MASK
    dest = ids >> log_loc
    big = jnp.int32(1 << 20)
    masked = [jnp.where(dest == d, prio, big) for d in range(ep)]

    def bit_step(i, thr):
        cand = thr + (jnp.int32(1) << (PRIO_BITS - 1 - i))
        rows = [
            jnp.sum(jnp.where(masked[d] < cand[d:d + 1, :], 1.0, 0.0), axis=0, keepdims=True)
            for d in range(ep)
        ]
        cnt = jnp.sum(jnp.concatenate(rows, axis=0), axis=1, keepdims=True)
        return jnp.where(cnt <= float(capacity), cand, thr)

    thr = lax.fori_loop(0, PRIO_BITS, bit_step, jnp.zeros((ep, 1), jnp.int32))

    def kept_ids(i, p):
        lim = jnp.zeros_like(i)
        for d in range(ep):
            lim = jnp.where((i >> log_loc) == d, thr[d:d + 1, :], lim)
        return p < lim

    kept = kept_ids(ids, prio)
    r_all = jnp.where(kept, (ids & (n_loc - 1)) * ep + dest, -1)
    id_all = jnp.where(kept, ids, -1)
    own = own_ref[...]
    own_id = (own >> PRIO_BITS) ^ (me * n_loc)
    own_kept = kept_ids(own_id, own & PRIO_MASK)
    r_own = jnp.where(own_kept, (own_id & (n_loc - 1)) * ep + (own_id >> log_loc), -1)

    iota_all = lax.broadcasted_iota(jnp.int32, (n_all, tok), 0)
    iota_loc = lax.broadcasted_iota(jnp.int32, (n_loc, tok), 0)

    def indicator(rows, iota):
        hit = rows[0:1, :] == iota
        for k in range(1, kpad):
            hit = hit | (rows[k:k + 1, :] == iota)
        return jnp.where(hit, 1.0, 0.0)

    lane = lax.broadcasted_iota(jnp.int32, (n_all, 128), 1)
    cnt = jnp.zeros((n_all, 128), jnp.float32)
    mine = []
    for s in range(ep):
        rows = slice(kpad * s, kpad * (s + 1))
        a_s = indicator(r_all[rows], iota_all)
        cnt = jnp.where(lane == s, jnp.sum(a_s, axis=1, keepdims=True), cnt)
        mine.append(indicator(id_all[rows], iota_loc))
    a_mine = jnp.concatenate(mine, axis=0)
    a_tok = indicator(r_own, iota_all)
    upper = jnp.where(
        lax.broadcasted_iota(jnp.int32, (tok, tok), 0) < lax.broadcasted_iota(jnp.int32, (tok, tok), 1), 1.0, 0.0
    ).astype(jnp.bfloat16)
    both = jnp.concatenate([a_mine, a_tok], axis=0).astype(jnp.bfloat16)
    rank = jnp.dot(both, upper, preferred_element_type=jnp.float32)

    lane8 = lax.broadcasted_iota(jnp.int32, (ep, 128), 1)
    end = jnp.zeros((ep, 128), jnp.float32)
    bad = jnp.zeros((ep, 128), jnp.float32)
    n_rows, base_rows, base_tok = [], [], []
    first = {g[0]: c for c, g in enumerate(GROUPS)}
    last = {g[-1]: c for c, g in enumerate(GROUPS)}
    for e in range(n_loc):
        n_e = cnt[ep * e:ep * (e + 1)]
        base = end
        if e in first:
            base = jnp.maximum(end, float(STARTS[first[e]]))
        end = base + n_e
        bad = jnp.maximum(bad, jnp.where(n_e > float(SEG_MAX), 1.0, 0.0))
        tot = jnp.sum(n_e, axis=1, keepdims=True)
        bad = jnp.maximum(bad, jnp.where(tot > float(ROWS_MAX), 1.0, 0.0))
        if e in last:
            c = last[e]
            lim = STARTS[c + 1] + SPILL if c + 1 < len(STARTS) else BUCKET
            bad = jnp.maximum(bad, jnp.where(end > float(lim), 1.0, 0.0))
        n_rows.append(n_e[0:1, :])
        base_rows.append(base[0:1, :])
        base_tok.append(jnp.sum(jnp.where(lane8 == me, base, 0.0), axis=1, keepdims=True))
    n_mine = jnp.concatenate(n_rows, axis=0)
    base_mine = jnp.concatenate(base_rows, axis=0)
    off = jnp.zeros((n_loc, 128), jnp.float32)
    for s in range(ep):
        off = off + jnp.where(lane8 > s, n_mine[:, s:s + 1], 0.0)
    off_i = off.astype(jnp.int32)
    off_low = (off_i & 15).astype(jnp.float32)
    off_col = jnp.concatenate([off_low[:, s:s + 1] for s in range(ep)], axis=0)
    qx_ref[...] = jnp.where(a_mine > 0.5, rank[:ep * n_loc] + off_col, -1.0).astype(jnp.int32)
    base_col = jnp.concatenate(base_tok, axis=0)
    qt = jnp.where(a_tok > 0.5, rank[ep * n_loc:] + base_col, -1.0)
    qt_ref[...] = qt.T.astype(jnp.int32)
    bad_any = jnp.max(jnp.max(bad, axis=1, keepdims=True), axis=0, keepdims=True)
    tab_ref[...] = jnp.concatenate(
        [off_i, n_mine.astype(jnp.int32), base_mine.astype(jnp.int32),
         jnp.broadcast_to(bad_any, (n_loc, 128)).astype(jnp.int32)], axis=0)


def route(me, keys, own, ep, n_loc, capacity):
    tok = own.shape[1]
    vm = pl.BlockSpec(memory_space=pltpu.VMEM)
    return pl.pallas_call(
        functools.partial(route_kernel, ep, n_loc, capacity),
        out_shape=(
            jax.ShapeDtypeStruct((ep * n_loc, tok), jnp.int32),
            jax.ShapeDtypeStruct((tok, ep * n_loc), jnp.int32),
            jax.ShapeDtypeStruct((4 * n_loc, 128), jnp.int32),
        ),
        in_specs=[pl.BlockSpec(memory_space=pltpu.SMEM), vm, vm],
        out_specs=(vm, vm, vm),
        cost_estimate=pl.CostEstimate(flops=6_000_000_000, bytes_accessed=1 << 20, transcendentals=0),
        name="route",
    )(me, keys, own)


def experts_kernel(c, ep, tok, me_ref, tab_ref, qx_ref, *refs):
    group = GROUPS[c]
    start, width = window(c)
    n_e = len(group)
    is_first, is_last = c == 0, c == len(GROUPS) - 1
    refs = list(refs)
    b_hbm, w1_ref, w3_ref, w2_ref = refs[:4]
    del refs[:4]
    spill_in = None if is_first else refs.pop(0)
    outs = refs[:ep]
    del refs[:ep]
    spill_out = None if is_last else refs.pop(0)
    b_vmem, work, xb, ebf, ewin, stage, b_sem, o_sem, sp_sem = refs
    n_loc = 8
    i, f = pl.program_id(0), pl.program_id(1)
    n_f = pl.num_programs(1)
    e = group[0] + i
    me = me_ref[0]
    tail = 0 if is_last else SPILL
    hidden = xb.shape[1]

    def load(s):
        return pltpu.make_async_copy(b_hbm.at[pl.ds(s * tok, tok)], b_vmem.at[pl.ds(s * tok, tok)], b_sem.at[s])

    def load_spill():
        return pltpu.make_async_copy(spill_in, b_vmem.at[pl.ds(0, ep * SPILL)], b_sem.at[0])

    @pl.when((i == 0) & (f == 0))
    def _():
        for s in range(ep):
            load(s).start()
        ebf[:, ROWS_MAX:, :] = jnp.zeros((n_e, ebf.shape[1] - ROWS_MAX, hidden), jnp.bfloat16)

    @pl.when(f == 0)
    def _():
        work[...] = jnp.zeros_like(work)
        for s in range(ep):
            @pl.when(i == 0)
            def _():
                load(s).wait()
            o = tab_ref[e, s]
            o_al = pl.multiple_of((o >> 4) << 4, 16)
            q = qx_ref[pl.ds(s * n_loc + e, 1), :]
            hot = jnp.where(lax.broadcasted_iota(jnp.int32, (SEG_WIN, tok), 0) == q, 1.0, 0.0).astype(jnp.bfloat16)
            work[pl.ds(o_al, SEG_WIN), :] += jnp.dot(
                hot, b_vmem[s * tok:(s + 1) * tok, :], preferred_element_type=jnp.float32)
        xb[...] = work[:ROWS_MAX, :].astype(jnp.bfloat16)
        if not is_first:
            @pl.when(i == n_e - 1)
            def _():
                load_spill().start()

    x = xb[...]
    up_a = jnp.dot(x, w1_ref[0], preferred_element_type=jnp.float32)
    up_b = jnp.dot(x, w3_ref[0], preferred_element_type=jnp.float32)
    h = (jax.nn.silu(up_a) * up_b).astype(jnp.bfloat16)
    down = jnp.dot(h, w2_ref[0], preferred_element_type=jnp.float32)

    @pl.when(f == 0)
    def _():
        work[:ROWS_MAX, :] = down

    @pl.when((f > 0) & (f < n_f - 1))
    def _():
        work[:ROWS_MAX, :] += down

    @pl.when(f == n_f - 1)
    def _():
        ebf[i, :ROWS_MAX, :] = (work[:ROWS_MAX, :] + down).astype(jnp.bfloat16)

    @pl.when((f == n_f - 1) & (i == n_e - 1))
    def _():
        if not is_first:
            load_spill().wait()
        kw = n_e * SEG_WIN
        lane = lax.broadcasted_iota(jnp.int32, (1, kw), 1)
        for x_d in range(ep):
            s = me ^ x_d
            q = jnp.full((1, kw), -1, jnp.int32)
            for j, ex in enumerate(group):
                o, n, base = tab_ref[ex, s], tab_ref[n_loc + ex, s], tab_ref[2 * n_loc + ex, s]
                o_al = pl.multiple_of((o >> 4) << 4, 16)
                r = lane - (j * SEG_WIN + (o & 15))
                q = jnp.where((r >= 0) & (r < n), base - start + r, q)
                ewin[j * SEG_WIN:(j + 1) * SEG_WIN, :] = ebf[j, pl.ds(o_al, SEG_WIN), :]
            hot = jnp.where(lax.broadcasted_iota(jnp.int32, (width + tail, kw), 0) == q, 1.0, 0.0).astype(jnp.bfloat16)
            res = jnp.dot(hot, ewin[...], preferred_element_type=jnp.float32)
            slot = x_d % 2
            if x_d >= 2:
                pltpu.make_async_copy(stage.at[slot, :width], outs[x_d - 2], o_sem.at[slot]).wait()
                if not is_last:
                    pltpu.make_async_copy(stage.at[slot, width:], spill_out.at[pl.ds((x_d - 2) * SPILL, SPILL)], sp_sem.at[slot]).wait()
            if is_first:
                stage[slot] = res.astype(jnp.bfloat16)
            else:
                stage[slot, SPILL:, :] = res[SPILL:].astype(jnp.bfloat16)
                stage[slot, :SPILL, :] = (res[:SPILL] + b_vmem[x_d * SPILL:(x_d + 1) * SPILL, :].astype(jnp.float32)).astype(jnp.bfloat16)
            pltpu.make_async_copy(stage.at[slot, :width], outs[x_d], o_sem.at[slot]).start()
            if not is_last:
                pltpu.make_async_copy(stage.at[slot, width:], spill_out.at[pl.ds(x_d * SPILL, SPILL)], sp_sem.at[slot]).start()
        for x_d in range(ep - 2, ep):
            slot = x_d % 2
            pltpu.make_async_copy(stage.at[slot, :width], outs[x_d], o_sem.at[slot]).wait()
            if not is_last:
                pltpu.make_async_copy(stage.at[slot, width:], spill_out.at[pl.ds(x_d * SPILL, SPILL)], sp_sem.at[slot]).wait()


def experts(c, me, tab, qx, b_all, w1, w3, w2, spill, ep):
    group = GROUPS[c]
    _, width = window(c)
    n_e = len(group)
    hidden, ff = w1.shape[1], w1.shape[2]
    tok = b_all.shape[0] // ep
    is_first, is_last = c == 0, c == len(GROUPS) - 1
    tail = 0 if is_last else SPILL
    e0 = group[0]
    smem = pl.BlockSpec(memory_space=pltpu.SMEM)
    whole = lambda shape: pl.BlockSpec(shape, lambda i, f: (0,) * len(shape))
    hbm = pl.BlockSpec(memory_space=pl.ANY)
    in_specs = [
        smem, smem, whole(qx.shape), hbm,
        pl.BlockSpec((1, hidden, F_TILE), lambda i, f: (e0 + i, 0, f)),
        pl.BlockSpec((1, hidden, F_TILE), lambda i, f: (e0 + i, 0, f)),
        pl.BlockSpec((1, F_TILE, hidden), lambda i, f: (e0 + i, f, 0)),
    ]
    args = [me, tab, qx, b_all, w1, w3, w2]
    if not is_first:
        in_specs.append(hbm)
        args.append(spill)
    out_shape = [jax.ShapeDtypeStruct((width, hidden), jnp.bfloat16) for _ in range(ep)]
    if not is_last:
        out_shape.append(jax.ShapeDtypeStruct((ep * SPILL, hidden), jnp.bfloat16))
    rows = ROWS_MAX + SEG_WIN
    res = pl.pallas_call(
        functools.partial(experts_kernel, c, ep, tok),
        grid=(n_e, ff // F_TILE),
        in_specs=in_specs,
        out_specs=[hbm] * len(out_shape),
        out_shape=out_shape,
        scratch_shapes=[
            pltpu.VMEM((ep * tok, hidden), jnp.bfloat16),
            pltpu.VMEM((rows, hidden), jnp.float32),
            pltpu.VMEM((ROWS_MAX, hidden), jnp.bfloat16),
            pltpu.VMEM((n_e, rows, hidden), jnp.bfloat16),
            pltpu.VMEM((n_e * SEG_WIN, hidden), jnp.bfloat16),
            pltpu.VMEM((2, width + tail, hidden), jnp.bfloat16),
            pltpu.SemaphoreType.DMA((ep,)),
            pltpu.SemaphoreType.DMA((2,)),
            pltpu.SemaphoreType.DMA((2,)),
        ],
        compiler_params=pltpu.CompilerParams(
            dimension_semantics=("arbitrary", "arbitrary"), vmem_limit_bytes=66_000_000),
        cost_estimate=pl.CostEstimate(
            flops=n_e * 2 * ROWS_MAX * 3 * hidden * ff, bytes_accessed=n_e * 6 * hidden * ff, transcendentals=0),
        name=f"experts{c}",
    )(*args)
    res = list(res)
    return res[:ep], (None if is_last else res[ep])


def combine_kernel(c, ep, last, qt_ref, g_ref, acc_ref, *refs):
    blocks = refs[:ep]
    out_ref, wts, cat = refs[ep:]
    start, width = window(c)
    kk = ep * width
    tok = qt_ref.shape[0]
    n_all = qt_ref.shape[1]
    seen = GROUPS[c] if c == 0 else GROUPS[c - 1] + GROUPS[c]

    @pl.when(pl.program_id(0) == 0)
    def _():
        pos = qt_ref[...] - start
        col = lax.broadcasted_iota(jnp.int32, (tok, n_all), 1)
        row = jnp.where((pos >= 0) & (pos < width), pos + (col & (ep - 1)) * width, -1)
        gate = g_ref[...]
        for j in range(kk // 128):
            want = lax.broadcasted_iota(jnp.int32, (tok, 128), 1) + 128 * j
            w = jnp.zeros((tok, 128), jnp.float32)
            for x_d in range((128 * j) // width, (128 * j + 127) // width + 1):
                for e in seen:
                    k = e * ep + x_d
                    w = jnp.where(row[:, k:k + 1] == want, gate[:, k:k + 1], w)
            hi = w.astype(jnp.bfloat16)
            rest = w - hi.astype(jnp.float32)
            mid = rest.astype(jnp.bfloat16)
            low = (rest - mid.astype(jnp.float32)).astype(jnp.bfloat16)
            lanes = slice(128 * j, 128 * (j + 1))
            wts[0, :, lanes] = hi
            wts[1, :, lanes] = mid
            wts[2, :, lanes] = low

    for x_d in range(ep):
        cat[x_d * width:(x_d + 1) * width, :] = blocks[x_d][...]
    rows = cat[...]
    total = acc_ref[...]
    for part in range(3):
        total = total + jnp.dot(wts[part], rows, preferred_element_type=jnp.float32)
    out_ref[...] = total.astype(out_ref.dtype)


def combine(c, qt, gates, acc, blocks, ep):
    _, width = window(c)
    tok, hidden = acc.shape
    last = c == len(GROUPS) - 1
    n_tile = 512
    col = lambda rows: pl.BlockSpec((rows, n_tile), lambda n: (0, n))
    return pl.pallas_call(
        functools.partial(combine_kernel, c, ep, last),
        grid=(hidden // n_tile,),
        in_specs=[pl.BlockSpec(qt.shape, lambda n: (0, 0)), pl.BlockSpec(gates.shape, lambda n: (0, 0)), col(tok)]
        + [col(width)] * ep,
        out_specs=col(tok),
        out_shape=jax.ShapeDtypeStruct((tok, hidden), jnp.bfloat16 if last else jnp.float32),
        scratch_shapes=[
            pltpu.VMEM((3, tok, ep * width), jnp.bfloat16),
            pltpu.VMEM((ep * width, n_tile), jnp.bfloat16),
        ],
        compiler_params=pltpu.CompilerParams(dimension_semantics=("arbitrary",)),
        cost_estimate=pl.CostEstimate(
            flops=6 * tok * ep * width * hidden, bytes_accessed=2 * ep * width * hidden, transcendentals=0),
        name=f"combine{c}",
    )(qt, gates, acc, *blocks)


def solution(mesh):
    ep = mesh.shape['ep']
    tok_spec = P(('dp', 'ep'))
    expert_spec = P('ep')

    def device_fn(resid_in, expert_ids, priority, norm_gain, router_w, shared_w1, shared_w3, shared_w2, expert_w1, expert_w3, expert_w2):
        tok, top_k = expert_ids.shape
        n_loc = expert_w1.shape[0]
        n_all = n_loc * ep
        capacity = tok * top_k
        me = lax.axis_index('ep').astype(jnp.int32)
        me1 = me.reshape(1)

        key = (expert_ids << PRIO_BITS) | priority
        pad = jnp.full((8 - top_k, tok), ((n_all - 1) << PRIO_BITS) | PRIO_MASK, jnp.int32)
        own = jnp.concatenate([key.T, pad], axis=0)
        keys = lax.all_gather(own, 'ep', tiled=True)

        resid32 = resid_in.astype(jnp.float32)
        inv_rms = lax.rsqrt(jnp.mean(resid32 * resid32, axis=1, keepdims=True) + NORM_EPS)
        normed = (resid32 * inv_rms * norm_gain).astype(jnp.bfloat16)
        all_normed = lax.all_gather(normed, 'ep', tiled=True)

        qx, qt, tab = route(me1, keys, own, ep, n_loc, capacity)

        cols = jnp.arange(n_all, dtype=jnp.int32)
        real = ((cols % ep) ^ me) * n_loc + cols // ep
        perm = (jnp.arange(n_all, dtype=jnp.int32)[:, None] == real[None, :]).astype(jnp.bfloat16)
        router_x = jnp.dot(router_w, perm, preferred_element_type=jnp.float32).astype(jnp.bfloat16)
        gates = ROUTE_SCALE * jax.nn.softmax(jnp.dot(normed, router_x, preferred_element_type=jnp.float32), axis=1)

        up_a = jnp.dot(normed, shared_w1, preferred_element_type=jnp.float32)
        up_b = jnp.dot(normed, shared_w3, preferred_element_type=jnp.float32)
        hidden_act = (jax.nn.silu(up_a) * up_b).astype(jnp.bfloat16)
        shared_out = jnp.dot(hidden_act, shared_w2, preferred_element_type=jnp.float32).astype(jnp.bfloat16)
        acc0 = resid32 + shared_out.astype(jnp.float32)

        def fast(_):
            acc = acc0
            spill = None
            for c in range(len(GROUPS)):
                sends, spill = experts(c, me1, tab, qx, all_normed, expert_w1, expert_w3, expert_w2, spill, ep)
                blocks = [sends[0]] + [
                    lax.ppermute(sends[x], 'ep', [(i, i ^ x) for i in range(ep)]) for x in range(1, ep)
                ]
                acc = combine(c, qt, gates, acc, blocks, ep)
            return acc

        def slow(_):
            inv = jnp.dot(gates, perm.T.astype(jnp.float32), precision=lax.Precision.HIGHEST)
            return general_path(acc0, all_normed, expert_ids, priority, inv, me, expert_w1, expert_w3, expert_w2, ep)

        return lax.cond(tab[3 * n_loc, 0] == 0, fast, slow, 0)

    return jax.shard_map(device_fn, mesh=mesh, in_specs=(tok_spec, tok_spec, tok_spec, P(), P(), P(), P(), P(), expert_spec, expert_spec, expert_spec), out_specs=tok_spec, check_vma=False)
```
